512 devices in a mesh: rep: 2 (over y), cp: 32 (over z, core), tp: 8 (over x).
Axes of the slice: x: 8, y: 2, z: 16, core: 2. Of those that a mesh axis runs over, the one named last changes fastest.
The devices are a block of a 8x8x16 slice.
Arguments:
- queries: bfloat16 [16384, 8192], P(('rep', 'cp'), 'tp'), parts along dimension 0, may hold values from -16 to 16
- keys: bfloat16 [16384, 1024], P(('rep', 'cp'), 'tp'), parts along dimension 0, may hold values from -16 to 16
- values: bfloat16 [16384, 1024], P(('rep', 'cp'), 'tp'), parts along dimension 0, may hold values from -6 to 6
- segment_ids: int32 [16384], P(('rep', 'cp')), parts along dimension 0, may hold values from 0 to 31, never falling along the last dimension, each value on 1 to 6144 neighbouring positions
Outputs:
- attended: bfloat16 [16384, 8192], P(('rep', 'cp'), 'tp'), parts along dimension 0
The draws below stay inside these ranges and needn't reach their ends.
There are 2 independent parts, one for each index of `rep`. The reference program is written for one: setup_inputs(seed, part) draws one part's arguments, and reference() takes and returns one part's arrays. A program takes and returns all parts, laid end to end along the dimension named above; each array names one. Nothing has to cross between parts.
Inputs may be any that keep to these rules, and one draw needn't show every extreme that they name: `segment_ids`: segment ids never fall along the sequence of one part.
All inputs are finite; a program needn't handle non-finite values.
Results may differ from the reference program's by a relative error of at most 0.012.
Values may be sent and summed in bfloat16 or wider, within the bound.
No kernel may reach another device: no remote copies, remote signals or barrier semaphores. Data moves between devices by JAX's collectives and lax.ppermute only.
A program may use at most 64 MiB of HBM per device.

```python
import math
import jax
import jax.numpy as jnp
import numpy as np
from jax import lax

HEADS = 64
KV_HEADS = 8
HEAD_DIM = 128
TOK_DEV = 256
LENGTH = 8192
N_CP = 32


def drawn_pair(key):
    base = jax.random.fold_in(key, 31)
    key_q, key_k = jax.random.split(base, 2)
    query_all = jnp.clip(jax.random.normal(key_q, (LENGTH, HEADS, HEAD_DIM), jnp.float32), -4.0, 4.0)
    key_all = jnp.clip(jax.random.normal(key_k, (LENGTH, KV_HEADS, HEAD_DIM), jnp.float32), -4.0, 4.0)
    return (query_all.reshape(LENGTH, HEADS * HEAD_DIM), key_all.reshape(LENGTH, KV_HEADS * HEAD_DIM))


def draw_queries(key, part):
    return drawn_pair(key)[0].astype(jnp.bfloat16)


def draw_keys(key, part):
    return drawn_pair(key)[1].astype(jnp.bfloat16)


def steps_of(rng, extent, pieces, low, largest):
    loudness = 1.0
    for position, shards_of in pieces:
        heights = jax.random.uniform(jax.random.fold_in(jax.random.fold_in(rng, 6), position), (shards_of,), jnp.float32, low / len(pieces), largest / len(pieces))
        loudness = loudness * jnp.repeat(jnp.exp(heights), extent[position] // shards_of).reshape((-1,) + (1,) * (len(extent) - 1 - position))
    return loudness


def split_up(number_of, total, most, skew):
    weights = [(1 << 20) // math.isqrt(rank ** skew) + 1 for rank in range(2, number_of + 1)]
    spare, given = total - most - (number_of - 1), [1] * (number_of - 1)
    while spare > 0:
        free = [i for i in range(number_of - 1) if given[i] < most]
        whole, left = sum([weights[i] for i in free]), spare
        for i in free:
            addition = min(most - given[i], max(1, left * weights[i] // whole), spare)
            given[i] = given[i] + addition
            spare = spare - addition
    return np.array([most] + given)


def uneven(key, number_of, total, reach, skew):
    if number_of == 2:
        one = jax.random.randint(key, (), max(1, total - reach), min(reach, total - 1) + 1)
        return jnp.stack([one, total - one])
    tallies = jnp.asarray(split_up(number_of, total, reach, skew), jnp.int32)
    pairs = (number_of - 1) // 2
    source_of, sink = tallies[1:1 + 2 * pairs:2], tallies[2:2 + 2 * pairs:2]
    slack = jnp.minimum(source_of - 1, reach - sink)
    moved = jax.random.randint(jax.random.fold_in(key, 1), (pairs,), 0, 1 << 20) % (slack + 1)
    tallies = tallies.at[1:1 + 2 * pairs:2].set(source_of - moved).at[2:2 + 2 * pairs:2].set(sink + moved)
    return tallies[jax.random.permutation(jax.random.fold_in(key, 2), number_of)]


def centred(key, shape, spread, most, cuts=(), kind=jnp.bfloat16):
    values = jax.random.normal(key, shape, jnp.float32) * spread
    if len(cuts) > 0:
        values = steps_of(key, shape, cuts, -0.22, 0.18) * values
    return jnp.clip(values, min=-most, max=most).astype(kind)


def setup_inputs(seed: int = 0, part: int = 0) -> dict:
    splits = jax.random.split(jax.random.key(seed), 5)
    part_keys = jax.random.split(jax.random.fold_in(splits[4], part), 5)
    queries = draw_queries(jax.random.fold_in(jax.random.fold_in(splits[4], part), 71), part)
    keys = draw_keys(jax.random.fold_in(jax.random.fold_in(splits[4], part), 71), part)
    values = centred(part_keys[2], (LENGTH, KV_HEADS * HEAD_DIM), 1.0, 6.0, ((0, 32), (1, 8)))
    segment_ids = jnp.searchsorted(jnp.cumsum(uneven(part_keys[3], N_CP, LENGTH, TOK_DEV * N_CP * 3 // 4, 2)), jnp.arange(LENGTH), side="right").astype(jnp.int32)
    return dict(queries=queries, keys=keys, values=values, segment_ids=segment_ids)


rope_base = 500000.0

def rotate(vectors, positions):
    half = vectors.shape[-1] // 2
    freq = rope_base ** (-jnp.arange(half, dtype=jnp.float32) * 2.0 / vectors.shape[-1])
    angle = positions.astype(jnp.float32)[:, None] * freq[None, :]
    cosine = jnp.cos(angle)[:, None, :]
    sine = jnp.sin(angle)[:, None, :]
    first = vectors[..., :half]
    second = vectors[..., half:]
    return jnp.concatenate([first * cosine - second * sine, second * cosine + first * sine], axis=-1)

def reference(queries, keys, values, segment_ids):
    total_len = queries.shape[0]
    index = jnp.arange(total_len, dtype=jnp.int32)
    starts = jnp.searchsorted(segment_ids, segment_ids, side='left').astype(jnp.int32)
    positions = index - starts
    group = HEADS // KV_HEADS
    rot_q = rotate(queries.astype(jnp.float32).reshape(total_len, HEADS, HEAD_DIM), positions).astype(jnp.bfloat16)
    rot_k = rotate(keys.astype(jnp.float32).reshape(total_len, KV_HEADS, HEAD_DIM), positions).astype(jnp.bfloat16)
    key_heads = jnp.moveaxis(rot_k, 1, 0).astype(jnp.float32)
    value_heads = jnp.moveaxis(values.reshape(total_len, KV_HEADS, HEAD_DIM), 1, 0).astype(jnp.float32)
    block = math.gcd(total_len, 512)
    count = total_len // block
    query_blocks = rot_q.reshape(count, block, KV_HEADS, group, HEAD_DIM)
    scale = 1.0 / math.sqrt(HEAD_DIM)

    def one_block(packed):
        query_block, number = packed
        row_index = number * block + jnp.arange(block, dtype=jnp.int32)
        row_start = lax.dynamic_slice_in_dim(starts, (number * block).astype(jnp.int32), block)
        keep = (index[None, :] <= row_index[:, None]) & (index[None, :] >= row_start[:, None])
        per_head = jnp.moveaxis(query_block, 1, 0).astype(jnp.float32)

        def one_head(triple):
            query_head, key_head, value_head = triple
            scores = jnp.einsum('tjd,kd->jtk', query_head, key_head) * scale
            scores = jnp.where(keep[None], scores, -1e+30)
            top = lax.optimization_barrier(jnp.max(scores, axis=-1, keepdims=True))
            weights = jnp.where(keep[None], jnp.exp(scores - top), 0.0)
            totals = lax.optimization_barrier(jnp.sum(weights, axis=-1))
            weights_low = weights.astype(jnp.bfloat16).astype(jnp.float32)
            summed = jnp.einsum('jtk,kd->tjd', weights_low, value_head)
            return summed / jnp.transpose(totals)[:, :, None]
        outputs = lax.map(one_head, (per_head, key_heads, value_heads))
        return jnp.moveaxis(outputs, 0, 1)
    results = lax.map(one_block, (query_blocks, jnp.arange(count, dtype=jnp.int32)))
    return results.reshape(total_len, HEADS * HEAD_DIM).astype(jnp.bfloat16)
```

```python
import functools
import math

import jax
import jax.numpy as jnp
from jax import lax
from jax.experimental import pallas as pl
from jax.experimental.pallas import tpu as pltpu
from jax.sharding import PartitionSpec as P

HEAD_DIM = 128
ROPE_BASE = 500000.0
MASKED = -1e30
NO_TOP = -1e29
EXTRA = 16


VMEM = pl.BlockSpec(memory_space=pltpu.VMEM)
PARAMS = pltpu.CompilerParams(vmem_limit_bytes=16 * 1024 * 1024)


def rotated(x_t, cos_t, sin_t):
    half = HEAD_DIM // 2
    a, b = x_t[:half], x_t[half:]
    return jnp.concatenate([a * cos_t - b * sin_t, b * cos_t + a * sin_t], axis=0)


def pack_kv_kernel(k_ref, v_ref, ids_ref, cos_ref, sin_ref, out_ref):
    tok = k_ref.shape[0]
    k_t = k_ref[...].astype(jnp.float32).T
    out_ref[0:tok, :] = rotated(k_t, cos_ref[...], sin_ref[...]).T.astype(jnp.bfloat16)
    v_t = v_ref[...].astype(jnp.float32).T.astype(jnp.bfloat16)
    pieces = tok // 128
    for i in range(pieces):
        out_ref[tok + i * HEAD_DIM : tok + (i + 1) * HEAD_DIM, :] = v_t[:, i * 128 : (i + 1) * 128]
    ids = ids_ref[...]
    rows = [ids[:, i * 128 : (i + 1) * 128] for i in range(pieces)]
    out_ref[tok + pieces * HEAD_DIM :, :] = jnp.concatenate(
        rows * (EXTRA // pieces), axis=0
    ).astype(jnp.bfloat16)


def pack_q_kernel(q_ref, ids_ref, cos_ref, sin_ref, out_ref, *, heads):
    factor = math.log2(math.e) / math.sqrt(HEAD_DIM)
    cos_t = cos_ref[...] * factor
    sin_t = sin_ref[...] * factor
    for j in range(heads):
        x_t = q_ref[:, j * HEAD_DIM : (j + 1) * HEAD_DIM].astype(jnp.float32).T
        out_ref[j * HEAD_DIM : (j + 1) * HEAD_DIM, :] = rotated(x_t, cos_t, sin_t).astype(
            jnp.bfloat16
        )
    out_ref[heads * HEAD_DIM :, :] = jnp.broadcast_to(
        ids_ref[...], (EXTRA, ids_ref.shape[1])
    ).astype(jnp.bfloat16)


def attend(q_ref, kv_ref, state_ref, heads, tok, keep, fresh):
    k = kv_ref[0:tok, :]
    v_t = jnp.concatenate(
        [kv_ref[tok + i * HEAD_DIM : tok + (i + 1) * HEAD_DIM, :] for i in range(tok // 128)],
        axis=1,
    )
    left = jnp.concatenate([v_t, jnp.ones((16, tok), jnp.bfloat16)], axis=0)

    def score(j):
        return jnp.dot(
            k, q_ref[j * HEAD_DIM : (j + 1) * HEAD_DIM, :], preferred_element_type=jnp.float32
        )

    s_next = score(0)
    for j in range(heads):
        s = s_next
        if j + 1 < heads:
            s_next = score(j + 1)
        if keep is not None:
            s = jnp.where(keep, s, MASKED)
        top = jnp.max(s, axis=0, keepdims=True)
        if fresh:
            top = jnp.maximum(top, NO_TOP)
        else:
            old = state_ref[j, HEAD_DIM + 8 : HEAD_DIM + 9, :]
            top = jnp.maximum(top, old)
        p = jnp.exp2(s - top).astype(jnp.bfloat16)
        new = jnp.dot(left, p, preferred_element_type=jnp.float32)[: HEAD_DIM + 8]
        if not fresh:
            new = state_ref[j, : HEAD_DIM + 8, :] * jnp.exp2(old - top) + new
        state_ref[j, : HEAD_DIM + 8, :] = new
        state_ref[j, HEAD_DIM + 8 :, :] = jnp.broadcast_to(top, (8, tok))


def id_column(kv_ref, tok):
    pieces = tok // 128
    ids = kv_ref[tok + pieces * HEAD_DIM :, :].astype(jnp.float32)
    ids_t = ids.T
    return jnp.concatenate([ids_t[:, i : i + 1] for i in range(pieces)], axis=0)


def id_row(q_ref, heads):
    return q_ref[heads * HEAD_DIM :, :].astype(jnp.float32)[:1]


def init_kernel(parity_ref, q_ref, q2_ref, kv_ref, st_ref, st2_ref, *, heads, tok):
    column = id_column(kv_ref, tok)
    key_at = lax.broadcasted_iota(jnp.int32, (tok, tok), 0)
    row_at = lax.broadcasted_iota(jnp.int32, (tok, tok), 1)
    keep = (column == id_row(q_ref, heads)) & (key_at <= row_at)
    attend(q_ref, kv_ref, st_ref, heads, tok, keep, True)

    @pl.when(parity_ref[0] == 0)
    def _():
        attend(q2_ref, kv_ref, st2_ref, heads, tok, column == id_row(q2_ref, heads), True)

    @pl.when(parity_ref[0] != 0)
    def _():
        st2_ref[:, : HEAD_DIM + 8, :] = jnp.zeros((heads, HEAD_DIM + 8, tok), jnp.float32)
        st2_ref[:, HEAD_DIM + 8 :, :] = jnp.full((heads, 8, tok), NO_TOP, jnp.float32)


def stage_kernel(*refs, heads, tok, count):
    live_ref, q_ref, q2_ref = refs[:3]
    kv_refs = refs[3 : 3 + count]
    st_in, st2_in, st_ref, st2_ref = refs[3 + count :]
    pieces = tok // 128

    for number, kv_ref in enumerate(kv_refs):

        @pl.when(live_ref[number] != 0)
        def _(kv_ref=kv_ref):
            ids = kv_ref[tok + pieces * HEAD_DIM :, :].astype(jnp.float32)
            first, last = jnp.min(ids), jnp.max(ids)
            for q, st in ((q_ref, st_ref), (q2_ref, st2_ref)):
                row = id_row(q, heads)
                q_first, q_last = jnp.min(row), jnp.max(row)
                seen = last == q_first
                whole = first == q_last

                @pl.when(seen & whole)
                def _(q=q, st=st):
                    attend(q, kv_ref, st, heads, tok, None, False)

                @pl.when(seen & jnp.logical_not(whole))
                def _(q=q, st=st):
                    keep = id_column(kv_ref, tok) == id_row(q, heads)
                    attend(q, kv_ref, st, heads, tok, keep, False)


def merge_kernel(st_ref, st2_ref, out_ref, *, heads):
    low, high = HEAD_DIM, HEAD_DIM + 8
    for j in range(heads):
        top = st_ref[j, high : high + 1, :]
        top2 = st2_ref[j, high : high + 1, :]
        best = jnp.maximum(top, top2)
        w, w2 = jnp.exp2(top - best), jnp.exp2(top2 - best)
        total = st_ref[j, low : low + 1, :] * w + st2_ref[j, low : low + 1, :] * w2
        o_t = (st_ref[j, :low, :] * w + st2_ref[j, :low, :] * w2) / total
        out_ref[:, j * HEAD_DIM : (j + 1) * HEAD_DIM] = o_t.T.astype(jnp.bfloat16)


def body(queries, keys, values, segment_ids):
    tok = queries.shape[0]
    heads = queries.shape[1] // HEAD_DIM
    devices = lax.axis_size("cp")
    chips = devices // 2
    place = lax.axis_index("cp")
    chip, parity = place // 2, place % 2
    half = HEAD_DIM // 2
    shape = jax.ShapeDtypeStruct

    position = (place * tok + jnp.arange(tok, dtype=jnp.int32)).astype(jnp.float32)
    freq = ROPE_BASE ** (-jnp.arange(half, dtype=jnp.float32) * 2.0 / HEAD_DIM)
    angle = freq[:, None] * position[None, :]
    cos_t, sin_t = jnp.cos(angle), jnp.sin(angle)
    ids = segment_ids.astype(jnp.float32)[None, :]

    own = pl.pallas_call(
        pack_kv_kernel,
        out_shape=shape((2 * tok + EXTRA, HEAD_DIM), jnp.bfloat16),
        in_specs=[VMEM] * 5,
        out_specs=VMEM,
        compiler_params=PARAMS,
        name="pack_kv",
    )(keys, values, ids, cos_t, sin_t)

    hop = lambda d: [(2 * c + s, 2 * ((c + d) % chips) + s) for c in range(chips) for s in (0, 1)]
    swap = [(2 * c + s, 2 * c + 1 - s) for c in range(chips) for s in (0, 1)]

    q_own = pl.pallas_call(
        functools.partial(pack_q_kernel, heads=heads),
        out_shape=shape((heads * HEAD_DIM + EXTRA, tok), jnp.bfloat16),
        in_specs=[VMEM] * 4,
        out_specs=VMEM,
        compiler_params=PARAMS,
        name="pack_q",
    )(queries, ids, cos_t, sin_t)
    q_other = lax.ppermute(q_own, "cp", swap)

    state_shape = shape((heads, HEAD_DIM + 16, tok), jnp.float32)
    smem = pl.BlockSpec(memory_space=pltpu.SMEM)
    tile_flops = 4 * heads * tok * tok * HEAD_DIM
    state = pl.pallas_call(
        functools.partial(init_kernel, heads=heads, tok=tok),
        out_shape=(state_shape, state_shape),
        in_specs=[smem] + [VMEM] * 3,
        out_specs=(VMEM, VMEM),
        compiler_params=PARAMS,
        cost_estimate=pl.CostEstimate(flops=tile_flops, bytes_accessed=0, transcendentals=0),
        name="own_keys",
    )(parity[None], q_own, q_other, own)

    up_steps = chips // 2
    down_steps = chips - 1 - up_steps
    up = down = own
    for step in range(1, up_steps + 1):
        up = lax.ppermute(up, "cp", hop(1))
        pieces, live = [up], [chip >= step]
        if step <= down_steps:
            down = lax.ppermute(down, "cp", hop(-1))
            pieces.append(down)
            live.append(chip + step >= chips)
        count = len(pieces)
        state = pl.pallas_call(
            functools.partial(stage_kernel, heads=heads, tok=tok, count=count),
            out_shape=(state_shape, state_shape),
            in_specs=[smem] + [VMEM] * (4 + count),
            out_specs=(VMEM, VMEM),
            input_output_aliases={3 + count: 0, 4 + count: 1},
            compiler_params=PARAMS,
            cost_estimate=pl.CostEstimate(
                flops=tile_flops * count, bytes_accessed=0, transcendentals=0
            ),
            name="stage",
        )(jnp.stack(live).astype(jnp.int32), q_own, q_other, *pieces, *state)

    other = lax.ppermute(state[1], "cp", swap)
    return pl.pallas_call(
        functools.partial(merge_kernel, heads=heads),
        out_shape=shape((tok, heads * HEAD_DIM), jnp.bfloat16),
        in_specs=[VMEM] * 2,
        out_specs=VMEM,
        compiler_params=PARAMS,
        name="merge",
    )(state[0], other)


def solution(mesh):
    return jax.shard_map(
        body,
        mesh=mesh,
        in_specs=(
            P(("rep", "cp"), "tp"),
            P(("rep", "cp"), "tp"),
            P(("rep", "cp"), "tp"),
            P(("rep", "cp")),
        ),
        out_specs=P(("rep", "cp"), "tp"),
        check_vma=False,
    )
```

```python
import functools
import math

import jax
import jax.numpy as jnp
from jax import lax
from jax.experimental import pallas as pl
from jax.experimental.pallas import tpu as pltpu
from jax.sharding import PartitionSpec as P


HEAD_DIM = 128
ROPE_BASE = 500000.0
MASKED = -1e30
NO_TOP = -1e29
EXTRA = 16
MAX_DOCUMENT = 6144
DIRECT = 2


VMEM = pl.BlockSpec(memory_space=pltpu.VMEM)
HBM = pl.BlockSpec(memory_space=pltpu.HBM)
PARAMS = pltpu.CompilerParams(vmem_limit_bytes=16 * 1024 * 1024)


def rotated(x_t, cos_t, sin_t):
    half = HEAD_DIM // 2
    a, b = x_t[:half], x_t[half:]
    return jnp.concatenate([a * cos_t - b * sin_t, b * cos_t + a * sin_t], axis=0)


def pack_kv_kernel(k_hbm, v_hbm, ids_hbm, cos_ref, sin_ref, out_ref, k_ref, v_ref, ids_ref, sems):
    tok = k_ref.shape[0]
    copies = [
        pltpu.make_async_copy(source, target, sems.at[i])
        for i, (source, target) in enumerate(
            ((k_hbm, k_ref), (v_hbm, v_ref), (ids_hbm, ids_ref))
        )
    ]
    for copy in copies:
        copy.start()
    for copy in copies:
        copy.wait()
    k_t = k_ref[...].astype(jnp.float32).T
    out_ref[0:tok, :] = rotated(k_t, cos_ref[...], sin_ref[...]).T.astype(jnp.bfloat16)
    v_t = v_ref[...].astype(jnp.float32).T.astype(jnp.bfloat16)
    pieces = tok // 128
    for i in range(pieces):
        out_ref[tok + i * HEAD_DIM : tok + (i + 1) * HEAD_DIM, :] = v_t[:, i * 128 : (i + 1) * 128]
    ids = ids_ref[...].astype(jnp.float32)
    rows = [ids[:, i * 128 : (i + 1) * 128] for i in range(pieces)]
    out_ref[tok + pieces * HEAD_DIM :, :] = jnp.concatenate(
        rows * (EXTRA // pieces), axis=0
    ).astype(jnp.bfloat16)


def pack_q_kernel(q_hbm, ids_hbm, cos_ref, sin_ref, out_ref, q_ref, ids_ref, sems, *, heads):
    q_copy = pltpu.make_async_copy(q_hbm, q_ref, sems.at[0])
    ids_copy = pltpu.make_async_copy(ids_hbm, ids_ref, sems.at[1])
    q_copy.start()
    ids_copy.start()
    q_copy.wait()
    ids_copy.wait()
    factor = math.log2(math.e) / math.sqrt(HEAD_DIM)
    cos_t = cos_ref[...] * factor
    sin_t = sin_ref[...] * factor
    for j in range(heads):
        x_t = q_ref[:, j * HEAD_DIM : (j + 1) * HEAD_DIM].astype(jnp.float32).T
        out_ref[j * HEAD_DIM : (j + 1) * HEAD_DIM, :] = rotated(x_t, cos_t, sin_t).astype(
            jnp.bfloat16
        )
    out_ref[heads * HEAD_DIM :, :] = jnp.broadcast_to(
        ids_ref[...].astype(jnp.float32), (EXTRA, ids_ref.shape[1])
    ).astype(jnp.bfloat16)


def attend(q_ref, kv_ref, state_ref, heads, tok, keep, fresh):
    k = kv_ref[0:tok, :]
    v_t = jnp.concatenate(
        [kv_ref[tok + i * HEAD_DIM : tok + (i + 1) * HEAD_DIM, :] for i in range(tok // 128)],
        axis=1,
    )
    left = jnp.concatenate([v_t, jnp.ones((16, tok), jnp.bfloat16)], axis=0)

    def some(heads_now):
        scores = []
        for j in heads_now:
            at = j * HEAD_DIM
            at = pl.ds(at if isinstance(at, int) else pl.multiple_of(at, HEAD_DIM), HEAD_DIM)
            scores.append(jnp.dot(k, q_ref[at, :], preferred_element_type=jnp.float32))
        results = []
        for j, s in zip(heads_now, scores):
            if keep is not None:
                s = jnp.where(keep, s, MASKED)
            top = jnp.max(s, axis=0, keepdims=True)
            if fresh:
                top = jnp.maximum(top, NO_TOP)
                factor = None
            else:
                old = state_ref[j, HEAD_DIM + 8 : HEAD_DIM + 9, :]
                top = jnp.maximum(top, old)
                factor = jnp.exp2(old - top)
            p = jnp.exp2(s - top).astype(jnp.bfloat16)
            results.append((jnp.dot(left, p, preferred_element_type=jnp.float32), top, factor))
        for j, (new, top, factor) in zip(heads_now, results):
            new = new[: HEAD_DIM + 8]
            if factor is not None:
                new = state_ref[j, : HEAD_DIM + 8, :] * factor + new
            state_ref[j, : HEAD_DIM + 8, :] = new
            state_ref[j, HEAD_DIM + 8 :, :] = jnp.broadcast_to(top, (8, tok))

    if fresh or keep is None:
        some(range(heads))
    else:
        group = math.gcd(heads, 2)

        def step(i, carry):
            some([i * group + j for j in range(group)])
            return carry

        lax.fori_loop(0, heads // group, step, 0)


def id_column(kv_ref, tok):
    pieces = tok // 128
    ids = kv_ref[tok + pieces * HEAD_DIM :, :].astype(jnp.float32)
    ids_t = ids.T
    return jnp.concatenate([ids_t[:, i : i + 1] for i in range(pieces)], axis=0)


def id_row(q_ref, heads):
    return q_ref[heads * HEAD_DIM :, :].astype(jnp.float32)[:1]


def init_kernel(q_ref, q2_ref, kv_ref, st_ref, st2_ref, *, heads, tok):
    parity = lax.axis_index("cp") % 2
    column = id_column(kv_ref, tok)
    key_at = lax.broadcasted_iota(jnp.int32, (tok, tok), 0)
    row_at = lax.broadcasted_iota(jnp.int32, (tok, tok), 1)
    keep = (column == id_row(q_ref, heads)) & (key_at <= row_at)
    attend(q_ref, kv_ref, st_ref, heads, tok, keep, True)

    @pl.when(parity == 0)
    def _():
        attend(q2_ref, kv_ref, st2_ref, heads, tok, column == id_row(q2_ref, heads), True)

    @pl.when(parity != 0)
    def _():
        st2_ref[:, : HEAD_DIM + 8, :] = jnp.zeros((heads, HEAD_DIM + 8, tok), jnp.float32)
        st2_ref[:, HEAD_DIM + 8 :, :] = jnp.full((heads, 8, tok), NO_TOP, jnp.float32)


def stage_kernel(q_ref, q2_ref, kv_ref, _, __, st_ref, st2_ref, *, heads, tok, distance):
    @pl.when(lax.axis_index("cp") // 2 >= distance)
    def _():
        ids = kv_ref[tok + tok // 128 * HEAD_DIM :, :].astype(jnp.float32)
        first, last = jnp.min(ids), jnp.max(ids)
        for q, st in ((q_ref, st_ref), (q2_ref, st2_ref)):
            row = id_row(q, heads)
            q_first, q_last = jnp.min(row), jnp.max(row)
            seen = last == q_first
            whole = first == q_last

            @pl.when(seen & whole)
            def _(q=q, st=st):
                attend(q, kv_ref, st, heads, tok, None, False)

            @pl.when(seen & jnp.logical_not(whole))
            def _(q=q, st=st):
                keep = id_column(kv_ref, tok) == id_row(q, heads)
                attend(q, kv_ref, st, heads, tok, keep, False)


def merge_kernel(st_ref, st2_ref, out_ref, *, heads):
    low, high = HEAD_DIM, HEAD_DIM + 8
    for j in range(heads):
        top = st_ref[j, high : high + 1, :]
        top2 = st2_ref[j, high : high + 1, :]
        best = jnp.maximum(top, top2)
        w, w2 = jnp.exp2(top - best), jnp.exp2(top2 - best)
        total = st_ref[j, low : low + 1, :] * w + st2_ref[j, low : low + 1, :] * w2
        o_t = (st_ref[j, :low, :] * w + st2_ref[j, :low, :] * w2) / total
        out_ref[:, j * HEAD_DIM : (j + 1) * HEAD_DIM] = o_t.T.astype(jnp.bfloat16)


def routes(chips, tok):
    reach = min(chips - 1, -(-MAX_DOCUMENT // (2 * tok)))
    direct = [d for d in range(reach, reach - DIRECT, -1) if 2 * d > chips]
    return reach - len(direct), direct


def stages(line, direct):
    order = list(range(1, line + 1))
    for back, d in enumerate(reversed(direct)):
        order.insert(line - 1 - back, d)
    return order


def body(queries, keys, values, segment_ids):
    tok = queries.shape[0]
    heads = queries.shape[1] // HEAD_DIM
    devices = lax.axis_size("cp")
    chips = devices // 2
    place = lax.axis_index("cp")
    half = HEAD_DIM // 2
    shape = jax.ShapeDtypeStruct

    position = (place * tok + jnp.arange(tok, dtype=jnp.int32)).astype(jnp.float32)
    freq = ROPE_BASE ** (-jnp.arange(half, dtype=jnp.float32) * 2.0 / HEAD_DIM)
    angle = freq[:, None] * position[None, :]
    cos_t, sin_t = jnp.cos(angle), jnp.sin(angle)
    ids = segment_ids[None, :]

    own = pl.pallas_call(
        pack_kv_kernel,
        out_shape=shape((2 * tok + EXTRA, HEAD_DIM), jnp.bfloat16),
        in_specs=[HBM] * 3 + [VMEM] * 2,
        out_specs=VMEM,
        scratch_shapes=[
            pltpu.VMEM(keys.shape, keys.dtype),
            pltpu.VMEM(values.shape, values.dtype),
            pltpu.VMEM(ids.shape, ids.dtype),
            pltpu.SemaphoreType.DMA((3,)),
        ],
        compiler_params=PARAMS,
        name="pack_kv",
    )(keys, values, ids, cos_t, sin_t)

    def moved(d, first):
        return [(2 * c + s, 2 * (c + d) + s) for c in range(first, chips - d) for s in (0, 1)]

    swap = [(2 * c + s, 2 * c + 1 - s) for c in range(chips) for s in (0, 1)]

    q_own = pl.pallas_call(
        functools.partial(pack_q_kernel, heads=heads),
        out_shape=shape((heads * HEAD_DIM + EXTRA, tok), jnp.bfloat16),
        in_specs=[HBM] * 2 + [VMEM] * 2,
        out_specs=VMEM,
        scratch_shapes=[
            pltpu.VMEM(queries.shape, queries.dtype),
            pltpu.VMEM(ids.shape, ids.dtype),
            pltpu.SemaphoreType.DMA((2,)),
        ],
        compiler_params=PARAMS,
        name="pack_q",
    )(queries, ids, cos_t, sin_t)
    q_other = lax.ppermute(q_own, "cp", swap)

    state_shape = shape((heads, HEAD_DIM + 16, tok), jnp.float32)
    tile_flops = 4 * heads * tok * tok * HEAD_DIM
    state = pl.pallas_call(
        functools.partial(init_kernel, heads=heads, tok=tok),
        out_shape=(state_shape, state_shape),
        in_specs=[VMEM] * 3,
        out_specs=(VMEM, VMEM),
        compiler_params=PARAMS,
        cost_estimate=pl.CostEstimate(flops=tile_flops, bytes_accessed=0, transcendentals=0),
        name="own_keys",
    )(q_own, q_other, own)

    def stage(state, piece, distance):
        return pl.pallas_call(
            functools.partial(stage_kernel, heads=heads, tok=tok, distance=distance),
            out_shape=(state_shape, state_shape),
            in_specs=[VMEM] * 5,
            out_specs=(VMEM, VMEM),
            input_output_aliases={3: 0, 4: 1},
            compiler_params=PARAMS,
            cost_estimate=pl.CostEstimate(flops=tile_flops, bytes_accessed=0, transcendentals=0),
            name="stage",
        )(q_own, q_other, piece, *state)

    line, direct = routes(chips, tok)
    up = own
    arrived = {}
    for step in range(1, line + 1):
        up = lax.ppermute(up, "cp", moved(1, step - 1))
        arrived[step] = up
    for d in direct:
        arrived[d] = lax.ppermute(own, "cp", moved(d, 0))
    for d in stages(line, direct):
        state = stage(state, arrived[d], d)

    other = lax.ppermute(state[1], "cp", swap)
    return pl.pallas_call(
        functools.partial(merge_kernel, heads=heads),
        out_shape=shape((tok, heads * HEAD_DIM), jnp.bfloat16),
        in_specs=[VMEM] * 2,
        out_specs=VMEM,
        compiler_params=PARAMS,
        name="merge",
    )(state[0], other)


def solution(mesh):
    return jax.shard_map(
        body,
        mesh=mesh,
        in_specs=(
            P(("rep", "cp"), "tp"),
            P(("rep", "cp"), "tp"),
            P(("rep", "cp"), "tp"),
            P(("rep", "cp")),
        ),
        out_specs=P(("rep", "cp"), "tp"),
        check_vma=False,
    )
```
